32 devices in a mesh: dp: 8 (over z, x), tensor: 4 (over y, core).
Axes of the slice: x: 2, y: 2, z: 4, core: 2. Of those that a mesh axis runs over, the one named last changes fastest.
Arguments:
- inputs: bfloat16 [16, 1024, 768], P('dp', 'tensor'), may hold values from -6 to 6
- lengths: int32 [16], P('dp'), may hold values from 16 to 1000, as said below
- w_qkv: bfloat16 [768, 3, 768], P(None, None, 'tensor'), may hold values from -0.21875 to 0.21875
- b_query: bfloat16 [768], P('tensor'), may hold values from -3 to 3
- b_value: bfloat16 [768], P('tensor'), may hold values from -3 to 3
- w_out: bfloat16 [768, 768], P('tensor'), may hold values from -1.75 to 1.75
- b_out: bfloat16 [768], replicated, may hold values from -3 to 3
- gain_one: bfloat16 [768], replicated, may hold values from 0.5 to 1.5
- shift_one: bfloat16 [768], replicated, may hold values from -3 to 3
- w_up: bfloat16 [768, 3072], P(None, 'tensor'), may hold values from -0.21875 to 0.21875
- b_up: bfloat16 [3072], P('tensor'), may hold values from -3 to 3
- w_down: bfloat16 [3072, 768], P('tensor'), may hold values from -0.109375 to 0.109375
- b_down: bfloat16 [768], replicated, may hold values from -3 to 3
- gain_two: bfloat16 [768], replicated, may hold values from 0.5 to 1.5
- shift_two: bfloat16 [768], replicated, may hold values from -3 to 3
- cotangent: bfloat16 [16, 1024, 768], P('dp', 'tensor'), may hold values from -6 to 6
Outputs:
- output: bfloat16 [16, 1024, 768], P('dp', 'tensor')
- grad_input: bfloat16 [16, 1024, 768], P('dp', 'tensor')
- grad_w_qkv: float32 [768, 3, 768], P(None, None, 'tensor')
- grad_b_query: float32 [768], P('tensor')
- grad_b_value: float32 [768], P('tensor')
- grad_w_out: float32 [768, 768], P('tensor')
- grad_b_out: float32 [768], replicated
- grad_gain_one: float32 [768], replicated
- grad_shift_one: float32 [768], replicated
- grad_w_up: float32 [768, 3072], P(None, 'tensor')
- grad_b_up: float32 [3072], P('tensor')
- grad_w_down: float32 [3072, 768], P('tensor')
- grad_b_down: float32 [768], replicated
- grad_gain_two: float32 [768], replicated
- grad_shift_two: float32 [768], replicated
The draws below stay inside these ranges and needn't reach their ends.
Inputs may be any that keep to these rules, and one draw needn't show every extreme that they name: `lengths`: each sequence's number of real slots; later slots are padding; in each aligned block of 2 sequences (the sequences of one index of dp) at least one has more than 768 real slots; some sequence has exactly 1000 in every draw.
All inputs are finite; a program needn't handle non-finite values.
Results may differ from the reference program's by a relative error of at most 0.012.
The reference program's roundings to bfloat16 on the way count: a program that leaves them out, or rounds other values in their place, can miss the bound.
Values may be sent and summed in bfloat16 or wider, within the bound.
A program may use at most 128 MiB of HBM per device.

```python
import math
import jax
import jax.numpy as jnp
from jax import lax

D = 768
HEADS = 12
HEAD_DIM = 64
FF = 3072
L = 1024
SEQ_DEV = 2
SEQS = 16
LONGEST = 1000
SHORTEST = 16


def draw_lengths(key, part):
    first_key, second_key, third_key, fourth_key = jax.random.split(jax.random.fold_in(key, 17), 4)
    base_draw = jax.random.randint(first_key, (SEQS,), 0, 1025)
    cubed = base_draw * base_draw * base_draw // 1024
    lengths_drawn = SHORTEST + (LONGEST - SHORTEST) * cubed // 1048576
    block_count = SEQS // SEQ_DEV
    picked = jax.random.randint(third_key, (block_count,), 0, SEQ_DEV)
    long_lo = L - L // 4 + 1
    long_drawn = jax.random.randint(fourth_key, (SEQS,), long_lo, LONGEST + 1)
    seq_ids = jnp.arange(SEQS, dtype=jnp.int32)
    is_long = seq_ids % SEQ_DEV == jnp.repeat(picked, SEQ_DEV)
    lengths_drawn = jnp.where(is_long, long_drawn, lengths_drawn)
    chosen = jax.random.randint(second_key, (), 0, block_count) * SEQ_DEV + jax.random.randint(jax.random.fold_in(second_key, 5), (), 0, SEQ_DEV)
    return jnp.where(seq_ids == chosen, LONGEST, lengths_drawn).astype(jnp.int32)


def block_scale(own_key, dims, shards, least, top_value):
    loudness, own = 1.0, jax.random.fold_in(own_key, 6)
    for position, shards_of in shards:
        steps = jnp.exp(jax.random.uniform(jax.random.fold_in(own, position), (shards_of,), jnp.float32, least / len(shards), top_value / len(shards)))
        loudness = loudness * jnp.repeat(steps, dims[position] // shards_of).reshape([-1 if axis == position else 1 for axis in range(len(dims))])
    return loudness


def gaussian(own_key, extent, deviation, limit, shards=(), kind=jnp.bfloat16):
    level = block_scale(own_key, extent, shards, -0.22, 0.18) if shards else 1.0
    values = jax.random.normal(own_key, extent, jnp.float32) * deviation * level
    return jnp.minimum(jnp.maximum(values, -limit), limit).astype(kind)


def setup_inputs(seed: int = 0) -> dict:
    key_of = jax.random.split(jax.random.key(seed), 17)
    inputs = gaussian(key_of[0], (SEQS, L, D), 1.0, 6.0, ((0, 8), (1, 4)))
    lengths = draw_lengths(jax.random.fold_in(key_of[16], 71), 0)
    w_qkv = gaussian(key_of[2], (D, 3, D), D ** -0.5, 0.21875, ((2, 4),))
    b_query = gaussian(key_of[3], (D,), 0.5, 3.0, ((0, 4),))
    b_value = gaussian(key_of[4], (D,), 0.5, 3.0, ((0, 4),))
    w_out = gaussian(key_of[5], (D, D), (max(1, D // 64)) ** -0.5, 1.75, ((0, 4),))
    b_out = gaussian(key_of[6], (D,), 0.5, 3.0)
    gain_one = jnp.clip(1.0 + 0.1 * jax.random.normal(key_of[7], (D,), jnp.float32), 0.5, 1.5).astype(jnp.bfloat16)
    shift_one = gaussian(key_of[8], (D,), 0.5, 3.0)
    w_up = gaussian(key_of[9], (D, FF), D ** -0.5, 0.21875, ((1, 4),))
    b_up = gaussian(key_of[10], (FF,), 0.5, 3.0, ((0, 4),))
    w_down = gaussian(key_of[11], (FF, D), FF ** -0.5, 0.109375, ((0, 4),))
    b_down = gaussian(key_of[12], (D,), 0.5, 3.0)
    gain_two = jnp.clip(1.0 + 0.1 * jax.random.normal(key_of[13], (D,), jnp.float32), 0.5, 1.5).astype(jnp.bfloat16)
    shift_two = gaussian(key_of[14], (D,), 0.5, 3.0)
    cotangent = gaussian(key_of[15], (SEQS, L, D), 1.0, 6.0, ((0, 8), (1, 4)))
    return dict(inputs=inputs, lengths=lengths, w_qkv=w_qkv, b_query=b_query, b_value=b_value, w_out=w_out, b_out=b_out, gain_one=gain_one, shift_one=shift_one, w_up=w_up, b_up=b_up, w_down=w_down, b_down=b_down, gain_two=gain_two, shift_two=shift_two, cotangent=cotangent)


EPSILON = 1e-05
HIGHEST = lax.Precision.HIGHEST

@jax.custom_vjp
def low(v):
    return lax.optimization_barrier(v.astype(jnp.bfloat16)).astype(jnp.float32)

@jax.custom_vjp
def low_back(v):
    return v

def low_keep(v):
    return (low(v), None)

def low_pass(kept, grad):
    return (grad,)

def back_keep(v):
    return (v, None)

def back_low(kept, grad):
    return (low(grad),)
low.defvjp(low_keep, low_pass)
low_back.defvjp(back_keep, back_low)

def matmul_hi(left, right):
    return jnp.dot(left, right, precision=HIGHEST, preferred_element_type=jnp.float32)

def layer_norm(values, gain, shift):
    row_mean = lax.optimization_barrier(jnp.mean(values, axis=-1, keepdims=True))
    centered = values - row_mean
    variance = lax.optimization_barrier(jnp.mean(centered * centered, axis=-1, keepdims=True))
    return centered * lax.rsqrt(variance + EPSILON) * gain + shift

def gelu_tanh(values):
    return jax.nn.gelu(values, approximate=True)

def attend(seq_block):
    queries = seq_block[:, 0]
    key_rows = seq_block[:, 1]
    value_rows = seq_block[:, 2]
    scores = jnp.einsum('qhd,khd->hqk', queries, key_rows, precision=HIGHEST) * (1.0 / math.sqrt(HEAD_DIM))
    positions = jnp.arange(L, dtype=jnp.int32)
    causal = positions[:, None] >= positions[None, :]
    scores = low_back(jnp.where(causal[None], scores, -1000000000.0))
    prob_rows = low(jax.nn.softmax(scores, axis=-1))
    return jnp.einsum('hqk,khd->qhd', prob_rows, value_rows, precision=HIGHEST)

def forward(params, source, row_masks):
    w_qkv, b_query, b_value, w_out, b_out, gain_one, shift_one, w_up, b_up, w_down, b_down, gain_two, shift_two = params
    normed = low(layer_norm(source, gain_one, shift_one))
    joined = matmul_hi(normed, w_qkv.reshape(D, 3 * D)).reshape(-1, 3, D)
    qkv_bias = jnp.stack([b_query, jnp.zeros_like(b_query), b_value])
    joined = low_back(low(joined + qkv_bias[None]))
    per_seq = joined.reshape(-1, L, 3, HEADS, HEAD_DIM)
    attended = lax.map(jax.checkpoint(attend), per_seq)
    attended = low_back(low(attended.reshape(-1, D)))
    branch = low_back(matmul_hi(attended, w_out) + b_out)
    hidden = source + branch
    second = low(layer_norm(hidden, gain_two, shift_two))
    pre_act = low_back(matmul_hi(second, w_up) + b_up)
    active = low(gelu_tanh(pre_act))
    result = hidden + matmul_hi(active, w_down) + b_down
    return result * row_masks[:, None]

def add_trees(left, right):
    return left + right

def reference(inputs, lengths, w_qkv, b_query, b_value, w_out, b_out, gain_one, shift_one, w_up, b_up, w_down, b_down, gain_two, shift_two, cotangent):
    params = tuple((item.astype(jnp.float32) for item in (w_qkv, b_query, b_value, w_out, b_out, gain_one, shift_one, w_up, b_up, w_down, b_down, gain_two, shift_two)))
    slot_ids = jnp.arange(L, dtype=jnp.int32)
    row_masks = (slot_ids[None, :] < lengths[:, None]).astype(jnp.float32)
    group_count = SEQS // SEQ_DEV
    x_groups = inputs.astype(jnp.float32).reshape(group_count, SEQ_DEV * L, D)
    m_groups = row_masks.reshape(group_count, SEQ_DEV * L)
    c_groups = cotangent.astype(jnp.float32).reshape(group_count, SEQ_DEV * L, D)

    def scan_step(totals, scan_item):
        group_x, group_m, group_c = scan_item

        def local_fn(params_in, inputs_in):
            return forward(params_in, inputs_in, group_m)
        result, pull_back = jax.vjp(local_fn, params, group_x)
        grads, grad_in = pull_back(group_c)
        totals = jax.tree.map(add_trees, totals, grads)
        return (totals, (result, grad_in))
    zero_grads = jax.tree.map(jnp.zeros_like, params)
    totals, (out_rows, din_rows) = lax.scan(scan_step, zero_grads, (x_groups, m_groups, c_groups))
    output = out_rows.reshape(SEQS, L, D).astype(jnp.bfloat16)
    grad_input = din_rows.reshape(SEQS, L, D).astype(jnp.bfloat16)
    return (output, grad_input, totals[0], totals[1], totals[2], totals[3], totals[4], totals[5], totals[6], totals[7], totals[8], totals[9], totals[10], totals[11], totals[12])
```

```python
import functools
import math

import jax
import jax.numpy as jnp
from jax import lax
from jax.experimental import pallas as pl
from jax.experimental.pallas import tpu as pltpu
from jax.sharding import PartitionSpec as P

EPSILON = 1e-05

HEAD_DIM=64

def nt(a, b):
    return lax.dot_general(a, b, (((1,), (1,)), ((), ())), preferred_element_type=jnp.float32)


def nn(a, b):
    return lax.dot_general(a, b, (((1,), (0,)), ((), ())), preferred_element_type=jnp.float32)


def tn(a, b):
    return lax.dot_general(a, b, (((0,), (0,)), ((), ())), preferred_element_type=jnp.float32)


def attend_kernel(half, heads, flag_ref, q_ref, kv_ref, kvp_ref, out_ref, lse_ref):
    outer = flag_ref[0]
    is_outer = outer == 1
    start = pl.multiple_of(outer * half, half)
    row = lax.broadcasted_iota(jnp.int32, (half, half), 0)
    col = lax.broadcasted_iota(jnp.int32, (half, half), 1)
    causal = row >= col
    lane = lax.broadcasted_iota(jnp.int32, (half, 128), 1)
    lo, hi = pl.ds(0, half), pl.ds(half, half)
    sel = pl.ds(start, half)
    lse_lo = jnp.zeros((half, 128), jnp.float32)
    lse_hi = jnp.zeros((half, 128), jnp.float32)
    scale = jnp.bfloat16(0.125)
    for h in range(heads):
        c = pl.ds(h * HEAD_DIM, HEAD_DIM)
        q_lo, q_hi, q_var = q_ref[lo, c] * scale, q_ref[hi, c] * scale, q_ref[sel, c] * scale
        s_var = nt(q_var, kvp_ref[0, sel, c])
        s_lo = jnp.where(causal, nt(q_lo, kv_ref[0, lo, c]), -1e9)
        s_one = nt(q_hi, kv_ref[0, lo, c])
        s_two = nt(q_hi, kvp_ref[0, lo, c])
        s_top = jnp.where(causal, nt(q_hi, kv_ref[0, hi, c]), -1e9)
        m_var = jnp.max(s_var, axis=1, keepdims=True)
        m_lo = jnp.max(s_lo, axis=1, keepdims=True)
        m_hi = jnp.max(jnp.maximum(jnp.maximum(s_one, s_two), s_top), axis=1, keepdims=True)
        m_lo = jnp.where(is_outer, m_lo, jnp.maximum(m_lo, m_var))
        m_hi = jnp.where(is_outer, jnp.maximum(m_hi, m_var), m_hi)
        e_var = jnp.exp(s_var - jnp.where(is_outer, m_hi, m_lo))
        e_lo = jnp.exp(s_lo - m_lo)
        e_one, e_two, e_top = jnp.exp(s_one - m_hi), jnp.exp(s_two - m_hi), jnp.exp(s_top - m_hi)
        l_var = jnp.sum(e_var, axis=1, keepdims=True)
        o_var = nn(e_var.astype(jnp.bfloat16), kvp_ref[1, sel, c])
        l_lo = jnp.sum(e_lo, axis=1, keepdims=True)
        o_lo = nn(e_lo.astype(jnp.bfloat16), kv_ref[1, lo, c])
        l_hi = jnp.sum(e_one + e_two + e_top, axis=1, keepdims=True)
        o_hi = (
            nn(e_one.astype(jnp.bfloat16), kv_ref[1, lo, c])
            + nn(e_two.astype(jnp.bfloat16), kvp_ref[1, lo, c])
            + nn(e_top.astype(jnp.bfloat16), kv_ref[1, hi, c])
        )
        l_lo = jnp.where(is_outer, l_lo, l_lo + l_var)
        o_lo = jnp.where(is_outer, o_lo, o_lo + o_var)
        l_hi = jnp.where(is_outer, l_hi + l_var, l_hi)
        o_hi = jnp.where(is_outer, o_hi + o_var, o_hi)
        out_ref[lo, c] = (o_lo / l_lo).astype(jnp.bfloat16)
        out_ref[hi, c] = (o_hi / l_hi).astype(jnp.bfloat16)
        lse_lo = jnp.where(lane == h, m_lo + jnp.log(l_lo), lse_lo)
        lse_hi = jnp.where(lane == h, m_hi + jnp.log(l_hi), lse_hi)
    lse_ref[lo, :] = lse_lo
    lse_ref[hi, :] = lse_hi


def attend(flag, q, kv, kvp):
    rows, width = q.shape
    heads = width // HEAD_DIM
    vm = pl.BlockSpec(memory_space=pltpu.VMEM)
    return pl.pallas_call(
        functools.partial(attend_kernel, rows // 2, heads),
        out_shape=(jax.ShapeDtypeStruct((rows, width), jnp.bfloat16), jax.ShapeDtypeStruct((rows, 128), jnp.float32)),
        in_specs=[pl.BlockSpec(memory_space=pltpu.SMEM), vm, vm, vm],
        out_specs=(vm, vm),
        cost_estimate=pl.CostEstimate(flops=heads * 10 * rows * rows // 4 * 256, bytes_accessed=rows * width * 16, transcendentals=heads * 5 * rows * rows // 4),
    )(flag, q, kv, kvp)


def attend_back_kernel(half, heads, flag_ref, q_ref, kv_ref, kvp_ref, att_ref, do_ref, lse_ref, dq_ref, dkv_ref, dkvp_ref):
    outer = flag_ref[0]
    is_outer = outer == 1
    start = pl.multiple_of(outer * half, half)
    key = lax.broadcasted_iota(jnp.int32, (half, half), 0)
    query = lax.broadcasted_iota(jnp.int32, (half, half), 1)
    causal = key <= query
    lane = lax.broadcasted_iota(jnp.int32, (2 * half, 128), 1)
    lo, hi = pl.ds(0, half), pl.ds(half, half)
    sel = pl.ds(start, half)
    scale = jnp.bfloat16(0.125)
    stats = lse_ref[...]
    for h in range(heads):
        c = pl.ds(h * HEAD_DIM, HEAD_DIM)
        prod = att_ref[:, c].astype(jnp.float32) * do_ref[:, c].astype(jnp.float32)
        stats = jnp.where(lane == 8 + h, jnp.sum(prod, axis=1, keepdims=True), stats)
    stats = stats.T

    def block(q, do, lse, delta, k, v, masked):
        p = jnp.exp(nt(k, q) - lse)
        if masked:
            p = jnp.where(causal, p, 0.0)
        ds = (p * (nt(v, do) - delta)).astype(jnp.bfloat16)
        return nn(p.astype(jnp.bfloat16), do), nn(ds, q), tn(ds, k)

    for h in range(heads):
        c = pl.ds(h * HEAD_DIM, HEAD_DIM)
        lse, delta = stats[h : h + 1, :], stats[8 + h : 9 + h, :]
        lse_lo, lse_hi, delta_lo, delta_hi = lse[:, :half], lse[:, half:], delta[:, :half], delta[:, half:]
        q_lo, q_hi, q_var = q_ref[lo, c] * scale, q_ref[hi, c] * scale, q_ref[sel, c] * scale
        do_lo, do_hi, do_var = do_ref[lo, c], do_ref[hi, c], do_ref[sel, c]
        lse_var, delta_var = jnp.where(is_outer, lse_hi, lse_lo), jnp.where(is_outer, delta_hi, delta_lo)
        dv_lo, dk_lo, dq_lo = block(q_lo, do_lo, lse_lo, delta_lo, kv_ref[0, lo, c], kv_ref[1, lo, c], True)
        dv_one, dk_one, dq_one = block(q_hi, do_hi, lse_hi, delta_hi, kv_ref[0, lo, c], kv_ref[1, lo, c], False)
        dv_two, dk_two, dq_two = block(q_hi, do_hi, lse_hi, delta_hi, kvp_ref[0, lo, c], kvp_ref[1, lo, c], False)
        dv_top, dk_top, dq_top = block(q_hi, do_hi, lse_hi, delta_hi, kv_ref[0, hi, c], kv_ref[1, hi, c], True)
        dv_var, dk_var, dq_var = block(q_var, do_var, lse_var, delta_var, kvp_ref[0, sel, c], kvp_ref[1, sel, c], False)
        dq_hi = dq_one + dq_two + dq_top
        dq_ref[lo, c] = (jnp.where(is_outer, dq_lo, dq_lo + dq_var) * 0.125).astype(jnp.bfloat16)
        dq_ref[hi, c] = (jnp.where(is_outer, dq_hi + dq_var, dq_hi) * 0.125).astype(jnp.bfloat16)
        dkv_ref[0, lo, c] = dk_lo + dk_one
        dkv_ref[1, lo, c] = dv_lo + dv_one
        dkv_ref[0, hi, c] = dk_top
        dkv_ref[1, hi, c] = dv_top
        dkvp_ref[0, lo, c] = jnp.where(is_outer, dk_two, dk_two + dk_var).astype(jnp.bfloat16)
        dkvp_ref[1, lo, c] = jnp.where(is_outer, dv_two, dv_two + dv_var).astype(jnp.bfloat16)
        dkvp_ref[0, hi, c] = jnp.where(is_outer, dk_var, 0.0).astype(jnp.bfloat16)
        dkvp_ref[1, hi, c] = jnp.where(is_outer, dv_var, 0.0).astype(jnp.bfloat16)


def attend_back(flag, q, kv, kvp, att, grad_att, lse):
    rows, width = q.shape
    heads = width // HEAD_DIM
    vm = pl.BlockSpec(memory_space=pltpu.VMEM)
    return pl.pallas_call(
        functools.partial(attend_back_kernel, rows // 2, heads),
        out_shape=(
            jax.ShapeDtypeStruct((rows, width), jnp.bfloat16),
            jax.ShapeDtypeStruct((2, rows, width), jnp.float32),
            jax.ShapeDtypeStruct((2, rows, width), jnp.bfloat16),
        ),
        in_specs=[pl.BlockSpec(memory_space=pltpu.SMEM)] + [vm] * 6,
        out_specs=(vm, vm, vm),
        cost_estimate=pl.CostEstimate(flops=heads * 25 * rows * rows // 4 * 256, bytes_accessed=rows * width * 30, transcendentals=heads * 5 * rows * rows // 4),
    )(flag, q, kv, kvp, att, grad_att, lse)


def swap(values, axis, bits):
    count = lax.axis_size(axis)
    return lax.ppermute(values, axis, [(i, i ^ bits) for i in range(count)])


def norm_rows(values):
    row_mean = jnp.mean(values, axis=-1, keepdims=True)
    centered = values - row_mean
    inverse = lax.rsqrt(jnp.mean(centered * centered, axis=-1, keepdims=True) + EPSILON)
    return centered * inverse, inverse


def norm_back(incoming, unit_rows, inverse, gain):
    scaled = incoming * gain
    part_sum = scaled - jnp.mean(scaled, axis=-1, keepdims=True)
    part_sum = part_sum - unit_rows * jnp.mean(scaled * unit_rows, axis=-1, keepdims=True)
    return part_sum * inverse


def gelu_tanh(values):
    return jax.nn.gelu(values, approximate=True)


def shards_of(weight):
    near = swap(weight, "tensor", 1)
    far = swap(weight, "tensor", 2)
    return [weight, near, far, swap(far, "tensor", 1)]


def reduce_shards(part):
    low = [part(k).astype(jnp.bfloat16) for k in (1, 3)]
    near = [swap(value, "tensor", 1).astype(jnp.float32) for value in low]
    far = swap((part(2) + near[1]).astype(jnp.bfloat16), "tensor", 2).astype(jnp.float32)
    return reduce_dp(part(0) + near[0] + far)


def reduce_dp(total):
    steps = int(math.log2(lax.axis_size("dp")))
    place = lax.axis_index("dp")
    for step in range(steps):
        halves = total.reshape(2, total.shape[0] // 2, *total.shape[1:])
        bit = (place >> step) & 1
        sent = lax.dynamic_index_in_dim(halves, 1 - bit, 0, keepdims=False).astype(jnp.bfloat16)
        kept = lax.dynamic_index_in_dim(halves, bit, 0, keepdims=False)
        total = kept + swap(sent, "dp", 1 << step).astype(jnp.float32)
    total = total.astype(jnp.bfloat16)
    for step in reversed(range(steps)):
        bit = (place >> step) & 1
        other = swap(total, "dp", 1 << step)
        first, last = jnp.where(bit == 0, total, other), jnp.where(bit == 0, other, total)
        total = jnp.concatenate([first, last], axis=0)
    return total.astype(jnp.float32)


def reduce_all(values):
    for axis in ("tensor", "dp"):
        for step in range(int(math.log2(lax.axis_size(axis)))):
            values = values + swap(values, axis, 1 << step)
    return values


def absolute(slots, place):
    slots = jnp.where(place & 1 == 1, slots[jnp.array([1, 0, 3, 2])], slots)
    return jnp.where(place & 2 == 2, slots[jnp.array([2, 3, 0, 1])], slots)


def own_row(rows, place):
    return lax.dynamic_index_in_dim(rows, place, 0, keepdims=False)


def per_device(
    inputs, lengths, w_qkv, b_query, b_value, w_out, b_out, gain_one, shift_one,
    w_up, b_up, w_down, b_down, gain_two, shift_two, cotangent,
):
    f32, low = jnp.float32, jnp.bfloat16
    _, quarter, width = inputs.shape
    local = w_out.shape[0]
    slots = range(4)
    place = lax.axis_index("tensor")
    chip = place >> 1
    outer = ((place == 0) | (place == 3)).astype(jnp.int32)
    first_quarter = jnp.minimum(place, 3 - place)
    here = (jnp.arange(2, dtype=jnp.int32) == chip)[:, None, None]

    def to_chip(values):
        give = lax.dynamic_index_in_dim(values, 1 - chip, 0, keepdims=False)
        return jnp.where(here, values, swap(give, "tensor", 3)[None])

    rows_in = to_chip(inputs).reshape(-1, width)
    w_qkv_own = jnp.transpose(w_qkv, (1, 0, 2))
    qkv_s = shards_of(w_qkv_own)
    biases = jnp.stack([b_query, b_value]).astype(f32)
    bias_s = shards_of(biases)
    out_s = shards_of(w_out)
    up_s = shards_of(w_up)
    up_bias_s = shards_of(b_up.astype(f32))
    down_s = shards_of(w_down)
    rows_cot = to_chip(cotangent).reshape(-1, width)

    slot_ids = jnp.arange(quarter, dtype=jnp.int32)
    positions = jnp.concatenate([first_quarter * quarter + slot_ids, (3 - first_quarter) * quarter + slot_ids])
    row_mask = (positions < own_row(lengths, chip)).astype(f32)[:, None]
    grad_out = rows_cot.astype(f32) * row_mask
    grad_low = grad_out.astype(low)

    source = rows_in.astype(f32)
    gain_first, gain_second = gain_one.astype(f32), gain_two.astype(f32)
    unit_one, inv_one = norm_rows(source)
    normed = (unit_one * gain_first + shift_one.astype(f32)).astype(low)
    flag = outer[None]
    q_s, kv_s = [], []
    for k in slots:
        q = jnp.dot(normed, qkv_s[k][0], preferred_element_type=f32) + bias_s[k][0]
        key = jnp.dot(normed, qkv_s[k][1], preferred_element_type=f32)
        value = jnp.dot(normed, qkv_s[k][2], preferred_element_type=f32) + bias_s[k][1]
        q_s.append(q.astype(low))
        kv_s.append(jnp.stack([key.astype(low), value.astype(low)]))
    moved = [swap(kv_s[k], "tensor", 1) for k in slots]
    kvp_s = [moved[k ^ 1] for k in slots]
    att_s, lse_s = zip(*[attend(flag, q_s[k], kv_s[k], kvp_s[k]) for k in slots])
    branch = sum(jnp.dot(att_s[k], out_s[k], preferred_element_type=f32) for k in slots)
    hidden = source + branch + b_out.astype(f32)
    unit_two, inv_two = norm_rows(hidden)
    second = (unit_two * gain_second + shift_two.astype(f32)).astype(low)
    pre_s = [jnp.dot(second, up_s[k], preferred_element_type=f32) + up_bias_s[k] for k in slots]
    active_s = [gelu_tanh(pre).astype(low) for pre in pre_s]
    mlp = sum(jnp.dot(active_s[k], down_s[k], preferred_element_type=f32) for k in slots)
    output = ((hidden + mlp + b_down.astype(f32)) * row_mask).astype(low)
    output = to_chip(output.reshape(2, quarter, width))

    grad_w_down = reduce_shards(lambda k: tn(active_s[k], grad_low))
    grad_pre_s = []
    for k in slots:
        _, pull = jax.vjp(gelu_tanh, pre_s[k])
        grad_pre_s.append(pull(nt(grad_low, down_s[k]))[0].astype(low))
    grad_w_up = reduce_shards(lambda k: tn(second, grad_pre_s[k]))
    grad_second = sum(nt(grad_pre_s[k], up_s[k]) for k in slots)
    grad_hidden = grad_out + norm_back(grad_second, unit_two, inv_two, gain_second)
    grad_branch = grad_hidden.astype(low)
    grad_w_out = reduce_shards(lambda k: tn(att_s[k], grad_branch))
    up_sums = jnp.stack([jnp.sum(grad_pre_s[k].astype(f32), axis=0) for k in slots])
    early = jnp.concatenate(
        [
            absolute(up_sums, place),
            jnp.stack(
                [
                    jnp.sum(grad_out, axis=0),
                    jnp.sum(grad_branch.astype(f32), axis=0),
                    jnp.sum(grad_second * unit_two, axis=0),
                    jnp.sum(grad_second, axis=0),
                ]
            ).reshape(-1, up_sums.shape[1]),
        ]
    )
    early = reduce_all(early)
    grad_b_up = own_row(early[:4], place)
    grad_b_down, grad_b_out, grad_gain_two, grad_shift_two = early[4:].reshape(4, width)

    back_s = []
    for k in slots:
        grad_att = nt(grad_branch, out_s[k]).astype(low)
        back_s.append(attend_back(flag, q_s[k], kv_s[k], kvp_s[k], att_s[k], grad_att, lse_s[k]))
    moved = [swap(back_s[k][2], "tensor", 1) for k in slots]
    joined_s = []
    for k in slots:
        grad_kv = (back_s[k][1] + moved[k ^ 1].astype(f32)).astype(low)
        joined_s.append((back_s[k][0], grad_kv[0], grad_kv[1]))
    grad_w_qkv = reduce_shards(lambda k: jnp.stack([tn(normed, part) for part in joined_s[k]]).reshape(-1, local))
    grad_w_qkv = jnp.transpose(grad_w_qkv.reshape(3, width, local), (1, 0, 2))
    grad_first = sum(nt(joined_s[k][j], qkv_s[k][j]) for k in slots for j in range(3))
    grad_input = (grad_hidden + norm_back(grad_first, unit_one, inv_one, gain_first)).astype(low)
    grad_input = to_chip(grad_input.reshape(2, quarter, width))
    bias_sums = jnp.stack(
        [jnp.concatenate([jnp.sum(joined_s[k][j].astype(f32), axis=0) for j in (0, 2)]) for k in slots]
    )
    late = jnp.concatenate(
        [
            absolute(bias_sums, place).reshape(-1, width),
            jnp.stack([jnp.sum(grad_first * unit_one, axis=0), jnp.sum(grad_first, axis=0)]),
        ]
    )
    late = reduce_all(late)
    own_bias = own_row(late[:2].reshape(4, 2, local), place)
    return (
        output, grad_input, grad_w_qkv, own_bias[0], own_bias[1], grad_w_out, grad_b_out, late[2], late[3],
        grad_w_up, grad_b_up, grad_w_down, grad_b_down, grad_gain_two, grad_shift_two,
    )


def solution(mesh):
    in_specs = (
        P("dp", "tensor", None),
        P("dp"),
        P(None, None, "tensor"),
        P("tensor"),
        P("tensor"),
        P("tensor", None),
        P(),
        P(),
        P(),
        P(None, "tensor"),
        P("tensor"),
        P("tensor", None),
        P(),
        P(),
        P(),
        P("dp", "tensor", None),
    )
    out_specs = (
        P("dp", "tensor", None),
        P("dp", "tensor", None),
        P(None, None, "tensor"),
        P("tensor"),
        P("tensor"),
        P("tensor", None),
        P(),
        P(),
        P(),
        P(None, "tensor"),
        P("tensor"),
        P("tensor", None),
        P(),
        P(),
        P(),
    )
    return jax.shard_map(
        per_device, mesh=mesh, in_specs=in_specs, out_specs=out_specs, check_vma=False
    )
```
